128 devices in a mesh: section: 2 (over z_hi), row: 8 (over x, core), col: 8 (over y, z_lo).
Axes of the slice: x: 4, y: 4, z: 4 (z_hi: 2, z_lo: 2; z = z_hi * 2 + z_lo), core: 2. Of those that a mesh axis runs over, the one named last changes fastest.
Arguments:
- inputs: float32 [3, 128, 16384], P(None, None, ('row', 'col')), may hold values from -512 to 512
- weights: float32 [2, 8, 8, 256, 16384], P('section', None, 'col', None, 'row'), may hold values from -1 to 1
- norm_gain: float32 [2, 16384], P('section', ('row', 'col')), may hold values from 0.5 to 1.5
Outputs:
- section_outputs: float32 [2, 3, 128, 16384], P('section', None, None, ('row', 'col'))
The draws below stay inside these ranges and needn't reach their ends.
All inputs are finite; a program needn't handle non-finite values.
Results may differ from the reference program's by a relative error of at most 0.00036.
Values sent between devices are 32-bit elements; how exact they have to be, the bound alone decides.
No kernel may reach another device: no remote copies, remote signals or barrier semaphores. Data moves between devices by JAX's collectives and lax.ppermute only.
A program may use at most 128 MiB of HBM per device.

```python
import math
import jax
import jax.numpy as jnp
from jax import lax

D = 16384
B = 128
M = 3
LAYERS = 2
ROW_BLOCKS = 8
COL_BLOCKS = 8
PIECE = 256


offset_scale = 64.0


def shared_basis(key):
    raw_draw = jax.random.normal(jax.random.fold_in(key, 7103), (D, M * B), jnp.float32)
    basis_cols, upper_part = jnp.linalg.qr(raw_draw)
    return basis_cols


def draw_inputs(key, part):
    basis_cols = shared_basis(key)
    count = M * B
    mixing = jax.random.normal(jax.random.fold_in(key, 211), (count, count), jnp.float32) / math.sqrt(count)
    amplitude = jnp.ones((count, 1), jnp.float32)
    rough = jax.random.normal(jax.random.fold_in(key, 229), (count, D), jnp.float32)
    along = jnp.dot(mixing, basis_cols.T, precision=lax.Precision.HIGHEST)
    large = offset_scale * math.sqrt(D) * amplitude * along
    values = jnp.clip(large + rough, -512.0, 512.0)
    return values.reshape(M, B, D)


def draw_weights(key, part):
    basis_cols = shared_basis(key)
    matrices = []
    for level in range(LAYERS):
        layer_key = jax.random.fold_in(key, 401 + level)
        dense = jnp.clip(jax.random.normal(layer_key, (D, D), jnp.float32), -6.0, 6.0) / math.sqrt(D)
        inside = jnp.dot(basis_cols.T, dense, precision=lax.Precision.HIGHEST)
        matrix = dense - (1.0 - 1.0 / offset_scale) * jnp.dot(basis_cols, inside, precision=lax.Precision.HIGHEST)
        matrices.append(matrix.reshape(ROW_BLOCKS, COL_BLOCKS, PIECE, D))
    return jnp.stack(matrices)


def setup_inputs(seed: int = 0) -> dict:
    key_of = jax.random.split(jax.random.key(seed), 4)
    return {
        "inputs": draw_inputs(jax.random.fold_in(key_of[3], 71), 0),
        "weights": draw_weights(jax.random.fold_in(key_of[3], 71), 0),
        "norm_gain": jnp.clip(1.0 + 0.1 * jax.random.normal(key_of[2], (LAYERS, D), jnp.float32), 0.5, 1.5),
    }


def split_two(values):
    first = lax.optimization_barrier(values.astype(jnp.bfloat16))
    second = lax.optimization_barrier((values - first.astype(jnp.float32)).astype(jnp.bfloat16))
    return (first, second)

def widen(values):
    return values.astype(jnp.float32)

def layer(activations, matrix, gain):
    first, second = split_two(activations)
    sum_two = widen(first) + widen(second)
    sum_one = widen(first)
    width = matrix.shape[1]
    block_cols = width // 8

    def column_block(index):
        cols = lax.dynamic_slice_in_dim(matrix, (index * block_cols).astype(jnp.int32), block_cols, 1)
        wfirst, wsecond = split_two(cols)
        total = jnp.dot(sum_two.astype(jnp.float32), widen(wfirst).astype(jnp.float32), precision=lax.Precision.HIGHEST, preferred_element_type=jnp.float32)
        total = total + jnp.dot(sum_one.astype(jnp.float32), widen(wsecond).astype(jnp.float32), precision=lax.Precision.HIGHEST, preferred_element_type=jnp.float32)
        return total
    blocks = lax.map(column_block, jnp.arange(8, dtype=jnp.int32))
    summed = jnp.transpose(blocks, (1, 0, 2)).reshape(activations.shape[0], width)
    active = jax.nn.gelu(summed, approximate=True)
    squares = lax.optimization_barrier(jnp.sum(active * active, axis=1))
    scale = lax.rsqrt(squares / width + 1e-06)
    return active * scale[:, None] * gain[None, :]

def reference(inputs, weights, norm_gain):
    current = inputs.reshape(M * B, D)
    results = []
    for level in range(LAYERS):
        matrix = weights[level].reshape(D, D)
        branch = layer(current, matrix, norm_gain[level])
        results.append(branch.reshape(M, B, D))
        current = current + branch
    return jnp.stack(results)
```

```python
import jax
import jax.numpy as jnp
from jax import lax
from jax.experimental import pallas as pl
from jax.experimental.pallas import tpu as pltpu
from jax.sharding import PartitionSpec as P

CHUNKS = (128, 128, 128)
ORDERS = ((2, 1, 0), (1, 0, 2), (0, 2, 1))
D = 16384
F = 256
f32 = jnp.float32
bf16 = jnp.bfloat16


def ring_partner(pos, mask):
    if mask & 1:
        pos = pos ^ 1
    if mask & 2:
        pos = 3 - pos
    return pos


def row_partner(row, mask):
    return ring_partner(row // 2, mask & 3) * 2 + ((row % 2) ^ (mask >> 2))


def col_partner(col, mask):
    return ring_partner(col // 2, mask & 3) * 2 + ((col % 2) ^ (mask >> 2))


def row_swap(value, mask):
    return lax.ppermute(value, "row", [(r, row_partner(r, mask)) for r in range(8)])


def col_swap(value, mask):
    return lax.ppermute(value, "col", [(c, col_partner(c, mask)) for c in range(8)])


def node_swap(value, mask):
    pairs = []
    for r in range(8):
        for c in range(8):
            pairs.append((r * 8 + c, row_partner(r, mask >> 3) * 8 + col_partner(c, mask & 7)))
    return lax.ppermute(value, ("row", "col"), pairs)


def vmem():
    return pl.BlockSpec(memory_space=pltpu.VMEM)


def smem():
    return pl.BlockSpec(memory_space=pltpu.SMEM)


def call(body, name, outs, args, scratch=(), limit=4 << 20, scalars=0, flops=0):
    return pl.pallas_call(
        body,
        name=name,
        out_shape=[jax.ShapeDtypeStruct(s, t) for s, t in outs],
        in_specs=[smem()] * scalars + [vmem()] * (len(args) - scalars),
        out_specs=[vmem()] * len(outs),
        scratch_shapes=list(scratch),
        compiler_params=pltpu.CompilerParams(vmem_limit_bytes=limit),
        cost_estimate=pl.CostEstimate(flops=flops, transcendentals=0, bytes_accessed=0),
    )(*args)


def split_weights(table, weights):
    def body(t, w, one, two):
        def step(n, _):
            m = n // 16
            sub = n % 16
            source = t[m] * F + sub * 16
            target = m * F + sub * 16
            for k in range(8):
                col = pl.multiple_of(t[8 + k] * F, F)
                value = w[pl.ds(pl.multiple_of(source, 16), 16), pl.ds(col, F)]
                first = value.astype(bf16)
                spot = pl.ds(pl.multiple_of(target, 16), 16)
                one[spot, k * F : (k + 1) * F] = first
                two[spot, k * F : (k + 1) * F] = (value - first.astype(f32)).astype(bf16)
            return 0

        lax.fori_loop(0, 128, step, 0)

    shape = (2048, 2048)
    return call(body, "split_weights", [(shape, bf16)] * 2, (table, weights), scalars=1, flops=1 << 24)


def parts_of(rows):
    count = len(ORDERS)
    if count == 1:
        return [(0, rows)]
    size = (rows // count) // 8 * 8
    ends = [size * (i + 1) for i in range(count - 1)] + [rows]
    starts = [0] + ends[:-1]
    return list(zip(starts, ends))


def slot(k, order):
    bits = [(k >> d) & 1 for d in order]
    return bits[0], bits[1] * 2 + bits[2]


def rows_to_lanes(total, rows):
    folded = total[:, :128] + total[:, 128:]
    lanes = []
    for start in range(0, rows, 128):
        block = folded[start : start + 128]
        if block.shape[0] < 128:
            block = jnp.concatenate([block, jnp.zeros((128 - block.shape[0], 128), f32)], axis=0)
        lanes.append(jnp.sum(block.T, axis=0, keepdims=True))
    lanes.append(jnp.zeros((8 - len(lanes), 128), f32))
    return jnp.concatenate(lanes, axis=0)


def lanes_to_rows(lanes, rows):
    blocks = []
    for i, start in enumerate(range(0, rows, 128)):
        count = min(128, rows - start)
        block = jnp.broadcast_to(lanes[i : i + 1], (128, 128)).T[:count]
        blocks.append(jnp.concatenate([block, block], axis=1))
    return blocks[0] if len(blocks) == 1 else jnp.concatenate(blocks, axis=0)


def product(pieces, across, first_w, second_w, rows, second_layer):
    parts = parts_of(rows)
    extra = 8 if second_layer else 0

    def body(p0, p1, p2, p3, q, w1, w2, *rest):
        outs = rest[: 2 * len(ORDERS)]
        lhs, acc = rest[2 * len(ORDERS) :]
        total = None
        for m in range(8):
            ref = (p0, p1, p2, p3)[m] if m < 4 else q.at[m - 4]
            value = ref[:rows]
            if second_layer:
                total = value * value if total is None else total + value * value
                value = value * ref[rows : rows + 1]
            first = value.astype(bf16)
            lhs[:rows, m * F : (m + 1) * F] = first
            lhs[rows:, m * F : (m + 1) * F] = (value - first.astype(f32)).astype(bf16)

        def step(k, _):
            spot = pl.ds(pl.multiple_of(k * F, F), F)
            both = jnp.dot(lhs[...], w1[:, spot], preferred_element_type=f32)
            other = jnp.dot(lhs[:rows], w2[:, spot], preferred_element_type=f32)
            acc[k] = both[:rows] + both[rows:] + other
            return 0

        lax.fori_loop(0, 8, step, 0)
        for i, ((start, end), order) in enumerate(zip(parts, ORDERS)):
            for k in range(8):
                sent, place = slot(k, order)
                target = outs[2 * i + (0 if sent else 1)]
                target[place, : end - start] = acc[k, start:end]
        if second_layer:
            lanes = rows_to_lanes(total, rows)
            lanes = jnp.concatenate([lanes, jnp.zeros((8, 128), f32)], axis=1)
            start, end = parts[0]
            for k in range(4):
                outs[0][k, end - start :] = lanes
                outs[1][k, end - start :] = lanes

    shapes = []
    for i, (start, end) in enumerate(parts):
        size = end - start + (extra if i == 0 else 0)
        shapes += [((4, size, F), f32)] * 2
    return call(
        body,
        "product",
        shapes,
        (*pieces, across, first_w, second_w),
        scratch=[pltpu.VMEM((2 * rows, 2048), bf16), pltpu.VMEM((8, rows, F), f32)],
        limit=12 << 20,
        flops=6 * rows * 2048 * 2048,
    )


def add_stage(kept, arrived):
    count = len(kept)

    def body(*refs):
        for i in range(count):
            keep, got = refs[i], refs[count + i]
            send, rest = refs[2 * count + 2 * i], refs[2 * count + 2 * i + 1]
            half = keep.shape[0] // 2
            send[...] = keep[half:] + got[half:]
            rest[...] = keep[:half] + got[:half]

    shapes = []
    for k in kept:
        shapes += [((k.shape[0] // 2, *k.shape[1:]), f32)] * 2
    return call(body, "add_stage", shapes, (*kept, *arrived), flops=1 << 20)


def summed(bufs):
    for stage in range(3):
        sends, kept = bufs[0::2], bufs[1::2]
        arrived = [col_swap(s, 1 << order[stage]) for s, order in zip(sends, ORDERS)]
        if stage == 2:
            return kept, arrived
        bufs = add_stage(kept, arrived)


def gelu(z):
    return 0.5 * z * (1.0 + jnp.tanh(0.7978845608028654 * (z + 0.044715 * (z * z * z))))


def first_end(kept, arrived, gain, rows):
    parts = parts_of(rows)
    count = len(parts)

    def body(*refs):
        g = refs[2 * count]
        z, y = refs[2 * count + 1 :]
        for i, (start, end) in enumerate(parts):
            value = refs[i][0] + refs[count + i][0]
            z[start:end] = value
            y[start:end] = gelu(value)
        y[rows:] = jnp.broadcast_to(g[...], (8, F))

    return call(body, "first_end", [((rows, F), f32), ((rows + 8, F), f32)], (*kept, *arrived, gain), flops=1 << 22)


def second_end(section, kept, arrived, before, gain, rows):
    parts = parts_of(rows)
    count = len(parts)

    def body(sec, *refs):
        za, g = refs[2 * count : 2 * count + 2]
        out, squares = refs[2 * count + 2 :]
        first = parts[0][1]
        lanes = refs[0][0, first:, :128] + refs[count][0, first:, :128]
        scale = lax.rsqrt(lanes_to_rows(lanes, rows) / D + 1e-06)

        @pl.when(sec[0] == 0)
        def _():
            out[...] = gelu(za[...]) * scale * g[...]
            squares[...] = jnp.zeros((8, 128), f32)

        @pl.when(sec[0] != 0)
        def _():
            value = [refs[i][0, : end - start] + refs[count + i][0, : end - start] for i, (start, end) in enumerate(parts)]
            value = value[0] if count == 1 else jnp.concatenate(value, axis=0)
            y = gelu(za[...] + scale * value)
            squares[...] = rows_to_lanes(y * y, rows)
            out[...] = y * g[...]

    return call(
        body, "second_end", [((rows, F), f32), ((8, 128), f32)], (section, *kept, *arrived, before, gain), scalars=1, flops=1 << 22
    )


def finish(section, values, squares):
    count = len(values)

    def body(sec, *refs):
        out = refs[2 * count]
        start = 0
        for i in range(count):
            value, lanes = refs[i], refs[count + i]
            rows = value.shape[0]

            @pl.when(sec[0] == 0)
            def _():
                out[start : start + rows] = value[...]

            @pl.when(sec[0] != 0)
            def _():
                scale = lax.rsqrt(lanes_to_rows(lanes[...], rows) / D + 1e-06)
                out[start : start + rows] = value[...] * scale

            start += rows

    total = sum(v.shape[0] for v in values)
    return call(body, "finish", [((total, F), f32)], (section, *values, *squares), scalars=1, flops=1 << 20)[0]


def gathered(value):
    own = [value] + [row_swap(value, mask) for mask in (1, 2, 3)]
    across = row_swap(jnp.stack(own), 4)
    return own, across


def total_over_nodes(lanes):
    for masks in ((8, 16, 24), (1, 2, 3), (32, 4, 36)):
        lanes = lanes + sum(node_swap(lanes, m) for m in masks)
    return lanes


def shards(inputs, weights, norm_gain):
    section = lax.axis_index("section").astype(jnp.int32)
    row = lax.axis_index("row").astype(jnp.int32)
    col = lax.axis_index("col").astype(jnp.int32)
    places = [row_partner(row, m) for m in range(8)] + [col_partner(col, k) for k in range(8)]
    table = jnp.stack(places).astype(jnp.int32)
    sec = section.reshape(1)
    flat = inputs.reshape(-1, F)
    gain = norm_gain
    first_w, second_w = split_weights(table, weights.reshape(2048, 2048))

    start = 0
    before, branch = [], []
    for rows in CHUNKS:
        own, across = gathered(flat[start : start + rows])
        start += rows
        kept, arrived = summed(product(own, across, first_w, second_w, rows, False))
        z, y = first_end(kept, arrived, gain, rows)
        before.append(z)
        moved = lax.ppermute(y, "section", [(0, 1)])
        branch.append(jnp.where(section == 0, y, moved))
    values, squares = [], []
    for rows, z, y in zip(CHUNKS, before, branch):
        own, across = gathered(y)
        kept, arrived = summed(product(own, across, first_w, second_w, rows, True))
        value, square = second_end(sec, kept, arrived, z, gain, rows)
        values.append(value)
        squares.append(square)
    joined = total_over_nodes(jnp.concatenate(squares, axis=0))
    squares = [joined[8 * i : 8 * i + 8] for i in range(len(CHUNKS))]
    return finish(sec, values, squares).reshape(1, *inputs.shape)


def solution(mesh):
    placed = (
        P(None, None, ("row", "col")),
        P("section", None, "col", None, "row"),
        P("section", ("row", "col")),
    )
    return jax.shard_map(
        shards,
        mesh=mesh,
        in_specs=placed,
        out_specs=P("section", None, None, ("row", "col")),
        check_vma=False,
    )
```

```python
import jax
import jax.numpy as jnp
from jax import lax
from jax.experimental import pallas as pl
from jax.experimental.pallas import tpu as pltpu
from jax.sharding import PartitionSpec as P

CHUNKS = (128, 128, 128)
D = 16384
F = 256
f32 = jnp.float32
bf16 = jnp.bfloat16
CYCLE = ((4, 1, 2), (1, 2, 4), (2, 4, 1))
RING = ((1, 2), (2, 1))


def mask_of(place, dims):
    return sum(dim for i, dim in enumerate(dims) if (place >> (len(dims) - 1 - i)) & 1)


def ring_partner(pos, mask):
    if mask & 1:
        pos = pos ^ 1
    if mask & 2:
        pos = 3 - pos
    return pos


def col_partner(col, mask):
    return ring_partner(col // 2, mask & 3) * 2 + ((col % 2) ^ (mask >> 2))


def swap_rows(value, masks):
    pairs = [(r, ring_partner(r // 2, masks[r % 2]) * 2 + r % 2) for r in range(8)]
    return lax.ppermute(value, "row", pairs)


def swap_cores(value):
    return lax.ppermute(value, "row", [(r, r ^ 1) for r in range(8)])


def swap_cols(value, masks):
    pairs = [(r * 8 + c, r * 8 + col_partner(c, masks[r % 2])) for r in range(8) for c in range(8)]
    return lax.ppermute(value, ("row", "col"), pairs)


def vmem():
    return pl.BlockSpec(memory_space=pltpu.VMEM)


def smem():
    return pl.BlockSpec(memory_space=pltpu.SMEM)


def call(body, name, outs, args, scratch=(), limit=4 << 20, scalars=0, flops=0, specs=None):
    return pl.pallas_call(
        body,
        name=name,
        out_shape=[jax.ShapeDtypeStruct(s, t) for s, t in outs],
        in_specs=specs or [smem()] * scalars + [vmem()] * (len(args) - scalars),
        out_specs=[vmem()] * len(outs),
        scratch_shapes=list(scratch),
        compiler_params=pltpu.CompilerParams(vmem_limit_bytes=limit),
        cost_estimate=pl.CostEstimate(flops=flops, transcendentals=0, bytes_accessed=0),
    )(*args)


def split_weights(weights):
    block, slots = 128, 4
    count = 2048 // block
    per = F // block

    def body(w, one, two, buf, sems):
        row = lax.axis_index("row")
        x, core = row // 2, row % 2

        def piece(m):
            whose = jnp.where(m < 4, core, 1 - core)
            low, high = m % 2, (m // 2) % 2
            one_flip = jnp.where(whose == 0, low, high)
            two_flip = jnp.where(whose == 0, high, low)
            chip = jnp.where(one_flip == 1, x ^ 1, x)
            chip = jnp.where(two_flip == 1, 3 - chip, chip)
            return chip * 2 + whose

        def fetch(n):
            m = n // per
            source = pl.multiple_of(piece(m) * F + (n % per) * block, block)
            return pltpu.make_async_copy(w.at[pl.ds(source, block)], buf.at[n % slots], sems.at[n % slots])

        for n in range(slots - 1):
            fetch(n).start()

        def step(n, _):
            @pl.when(n + slots - 1 < count)
            def _():
                fetch(n + slots - 1).start()

            fetch(n).wait()

            def rows(i, _):
                value = buf[n % slots, pl.ds(pl.multiple_of(i * 16, 16), 16)]
                first = value.astype(bf16)
                spot = pl.ds(pl.multiple_of(n * block + i * 16, 16), 16)
                one[spot] = first
                two[spot] = (value - first.astype(f32)).astype(bf16)
                return 0

            lax.fori_loop(0, block // 16, rows, 0)
            return 0

        lax.fori_loop(0, count, step, 0)

    shape = (2048, 2048)
    return call(
        body,
        "split_weights",
        [(shape, bf16)] * 2,
        (pltpu.with_memory_space_constraint(weights, pltpu.HBM),),
        scratch=[pltpu.VMEM((slots, block, 2048), f32), pltpu.SemaphoreType.DMA((slots,))],
        specs=[pl.BlockSpec(memory_space=pltpu.HBM)],
        limit=6 << 20,
        flops=1 << 24,
    )


def rows_to_lanes(total, rows):
    folded = total[:, :128] + total[:, 128:]
    lanes = []
    for start in range(0, rows, 128):
        block = folded[start : start + 128]
        if block.shape[0] < 128:
            block = jnp.concatenate([block, jnp.zeros((128 - block.shape[0], 128), f32)], axis=0)
        lanes.append(jnp.sum(block.T, axis=0, keepdims=True))
    lanes.append(jnp.zeros((8 - len(lanes), 128), f32))
    return jnp.concatenate(lanes, axis=0)


def lanes_to_rows(lanes, rows):
    blocks = []
    for i, start in enumerate(range(0, rows, 128)):
        count = min(128, rows - start)
        block = jnp.broadcast_to(lanes[i : i + 1], (128, 128)).T[:count]
        blocks.append(jnp.concatenate([block, block], axis=1))
    return blocks[0] if len(blocks) == 1 else jnp.concatenate(blocks, axis=0)


def product(orders, own, across, first_w, second_w, start, rows, second_layer):
    extra = 8 if second_layer else 0

    def body(p, q, w1, w2, send, keep, lhs):
        core, col = lax.axis_index("row") % 2, lax.axis_index("col")

        def place(slot):
            mask = 0
            for i in range(3):
                dim = jnp.where(core == 0, orders[0][i], orders[1][i])
                mask = mask + ((slot >> (2 - i)) & 1) * dim
            y = col // 2
            y = jnp.where((mask & 1) == 1, y ^ 1, y)
            y = jnp.where((mask & 2) == 2, 3 - y, y)
            return y * 2 + ((col % 2) ^ (mask >> 2))

        total = None
        for m in range(8):
            ref = p.at[m] if m < 4 else q.at[m - 4]
            value = ref[start : start + rows]
            if second_layer:
                total = value * value if total is None else total + value * value
                value = value * ref[rows : rows + 1]
            first = value.astype(bf16)
            lhs[:rows, m * F : (m + 1) * F] = first
            lhs[rows:, m * F : (m + 1) * F] = (value - first.astype(f32)).astype(bf16)

        def step(k, _):
            for target, slot in ((send, k + 4), (keep, k)):
                spot = pl.ds(pl.multiple_of(place(slot) * F, F), F)
                both = jnp.dot(lhs[...], w1[:, spot], preferred_element_type=f32)
                other = jnp.dot(lhs[:rows], w2[:, spot], preferred_element_type=f32)
                target[k, :rows] = both[:rows] + both[rows:] + other
            return 0

        lax.fori_loop(0, 4, step, 0)
        if second_layer:
            lanes = rows_to_lanes(total, rows)
            lanes = jnp.concatenate([lanes, jnp.zeros((8, 128), f32)], axis=1)
            for k in range(4):
                send[k, rows:] = lanes
                keep[k, rows:] = lanes

    return call(
        body,
        "product",
        [((4, rows + extra, F), f32)] * 2,
        (own, across, first_w, second_w),
        scratch=[pltpu.VMEM((2 * rows, 2048), bf16)],
        limit=8 << 20,
        flops=6 * rows * 2048 * 2048,
    )


def add_halves(kept, arrived):
    half = kept.shape[0] // 2

    def body(keep, got, send, rest):
        send[...] = keep[half:] + got[half:]
        rest[...] = keep[:half] + got[:half]

    return call(body, "add_halves", [((half, *kept.shape[1:]), f32)] * 2, (kept, arrived), flops=1 << 20)


def summed(sent, kept, orders):
    for stage in range(3):
        arrived = swap_cols(sent, [order[stage] for order in orders])
        if stage == 2:
            return kept, arrived
        sent, kept = add_halves(kept, arrived)


def gelu(z):
    return 0.5 * z * (1.0 + jnp.tanh(0.7978845608028654 * (z + 0.044715 * (z * z * z))))


def first_end(kept, arrived, gain, rows):
    def body(p, q, g, z, y):
        value = p[0] + q[0]
        z[...] = value
        y[:rows] = gelu(value)
        y[rows:] = jnp.broadcast_to(g[...], (8, F))

    return call(body, "first_end", [((rows, F), f32), ((rows + 8, F), f32)], (kept, arrived, gain), flops=1 << 22)


def second_end(kept, arrived, before, gain, rows):
    def body(p, q, za, g, out, squares):
        section = lax.axis_index("section")
        lanes = (p[0, rows:] + q[0, rows:])[:, :128]
        scale = lax.rsqrt(lanes_to_rows(lanes, rows) / D + 1e-06)

        @pl.when(section == 0)
        def _():
            out[...] = gelu(za[...]) * scale * g[...]
            squares[...] = jnp.zeros((8, 128), f32)

        @pl.when(section != 0)
        def _():
            y = gelu(za[...] + scale * (p[0, :rows] + q[0, :rows]))
            squares[...] = rows_to_lanes(y * y, rows)
            out[...] = y * g[...]

    return call(
        body,
        "second_end",
        [((rows, F), f32), ((8, 128), f32)],
        (kept, arrived, before, gain),
        flops=1 << 22,
    )


def finish(values, lanes):
    count = len(values)
    sizes = [v.shape[0] for v in values]

    def body(*refs):
        section = lax.axis_index("section")
        lanes = refs[count]
        out = refs[count + 1]

        @pl.when(section == 0)
        def _():
            start = 0
            for ref, rows in zip(refs, sizes):
                out[start : start + rows] = ref[...]
                start += rows

        @pl.when(section != 0)
        def _():
            total = jnp.sum(lanes[...], axis=0, keepdims=True)
            start, place = 0, 0
            for ref, rows in zip(refs, sizes):
                width = -(-rows // 128)
                part = [total[:, (place + i) * 128 : (place + i + 1) * 128] for i in range(width)]
                scale = lax.rsqrt(lanes_to_rows(jnp.concatenate(part, axis=0), rows) / D + 1e-06)
                out[start : start + rows] = ref[...] * scale
                start += rows
                place += width

    return call(body, "finish", [((sum(sizes), F), f32)], (*values, lanes), flops=1 << 20)[0]


def gathered(value):
    first = swap_rows(value, [ring[0] for ring in RING])
    pair = jnp.stack([value, first])
    own = jnp.concatenate([pair, swap_rows(pair, [ring[1] for ring in RING])], axis=0)
    return own, swap_cores(own)


def chosen(own, moved):
    def body(a, b, out):
        out[...] = jnp.where(lax.axis_index("section") == 0, a[...], b[...])

    return call(body, "chosen", [(own.shape, f32)], (own, moved))[0]


def shards(inputs, weights, norm_gain):
    flat = inputs.reshape(-1, F)
    gain = norm_gain
    first_w, second_w = split_weights(weights.reshape(2048, 2048))
    orders = [(CYCLE[i % 3], CYCLE[(i + 1) % 3]) for i in range(len(CHUNKS))]

    before, branch = [], []
    gathers = []
    first = CHUNKS[0]
    gathers.append((gathered(flat[:first]), 0))
    if len(CHUNKS) > 1:
        rest = gathered(flat[first:])
        start = 0
        for rows in CHUNKS[1:]:
            gathers.append((rest, start))
            start += rows
    for i, rows in enumerate(CHUNKS):
        (own, across), start = gathers[i]
        sent, kept = product(orders[i], own, across, first_w, second_w, start, rows, False)
        z, y = first_end(*summed(sent, kept, orders[i]), gain, rows)
        before.append(z)
        moved = lax.ppermute(y, "section", [(0, 1)])
        branch.append(chosen(y, moved))
    values, squares = [], []
    for i, rows in enumerate(CHUNKS):
        own, across = gathered(branch[i])
        sent, kept = product(orders[i], own, across, first_w, second_w, 0, rows, True)
        value, square = second_end(*summed(sent, kept, orders[i]), before[i], gain, rows)
        values.append(value)
        squares.append(square[: -(-rows // 128)].reshape(1, -1))
    lanes = jnp.concatenate(squares, axis=1)
    lanes = lax.all_to_all(jnp.broadcast_to(lanes[None], (64, *lanes.shape)), ("row", "col"), 0, 0, tiled=True)
    return finish(values, lanes.reshape(64, -1)).reshape(1, *inputs.shape)


def solution(mesh):
    placed = (
        P(None, None, ("row", "col")),
        P("section", None, "col", None, "row"),
        P("section", ("row", "col")),
    )
    return jax.shard_map(
        shards,
        mesh=mesh,
        in_specs=placed,
        out_specs=P("section", None, None, ("row", "col")),
        check_vma=False,
    )
```

```python
import jax
import jax.numpy as jnp
from jax import lax
from jax.experimental import pallas as pl
from jax.experimental.pallas import tpu as pltpu
from jax.sharding import PartitionSpec as P


CHUNKS = (128, 128, 128)
D = 16384
F = 256
f32 = jnp.float32
bf16 = jnp.bfloat16
CYCLE = ((4, 1, 2), (1, 2, 4), (2, 4, 1))
RING = ((1, 2), (2, 1))


def ring_partner(pos, mask):
    if mask & 1:
        pos = pos ^ 1
    if mask & 2:
        pos = 3 - pos
    return pos


def col_partner(col, mask):
    return ring_partner(col // 2, mask & 3) * 2 + ((col % 2) ^ (mask >> 2))


def swap_rows(value, masks):
    pairs = [(r, ring_partner(r // 2, masks[r % 2]) * 2 + r % 2) for r in range(8)]
    return lax.ppermute(value, "row", pairs)


def swap_cores(value):
    return lax.ppermute(value, "row", [(r, r ^ 1) for r in range(8)])


def swap_cols(value, masks):
    pairs = [(r * 8 + c, r * 8 + col_partner(c, masks[r % 2])) for r in range(8) for c in range(8)]
    return lax.ppermute(value, ("row", "col"), pairs)


def vmem():
    return pl.BlockSpec(memory_space=pltpu.VMEM)


def smem():
    return pl.BlockSpec(memory_space=pltpu.SMEM)


def call(body, outs, args, scratch=(), limit=4 << 20, scalars=0, flops=0, specs=None):
    return pl.pallas_call(
        body,
        out_shape=[jax.ShapeDtypeStruct(s, t) for s, t in outs],
        in_specs=specs or [smem()] * scalars + [vmem()] * (len(args) - scalars),
        out_specs=[vmem()] * len(outs),
        scratch_shapes=list(scratch),
        compiler_params=pltpu.CompilerParams(vmem_limit_bytes=limit),
        cost_estimate=pl.CostEstimate(flops=flops, transcendentals=0, bytes_accessed=0),
    )(*args)


def split_weights(weights, half):
    block, slots = 128, 4
    count = 1024 // block
    per = F // block

    def body(w, one, two, buf, sems):
        row = lax.axis_index("row")
        x, core = row // 2, row % 2

        def piece(m):
            whose = jnp.where(m < 4, core, 1 - core)
            low, high = m % 2, (m // 2) % 2
            one_flip = jnp.where(whose == 0, low, high)
            two_flip = jnp.where(whose == 0, high, low)
            chip = jnp.where(one_flip == 1, x ^ 1, x)
            chip = jnp.where(two_flip == 1, 3 - chip, chip)
            return chip * 2 + whose

        def fetch(n):
            m = n // per + 4 * half
            source = pl.multiple_of(piece(m) * F + (n % per) * block, block)
            return pltpu.make_async_copy(w.at[pl.ds(source, block)], buf.at[n % slots], sems.at[n % slots])

        for n in range(slots - 1):
            fetch(n).start()

        def step(n, _):
            @pl.when(n + slots - 1 < count)
            def _():
                fetch(n + slots - 1).start()

            fetch(n).wait()

            def rows(i, _):
                value = buf[n % slots, pl.ds(pl.multiple_of(i * 16, 16), 16)]
                first = value.astype(bf16)
                spot = pl.ds(pl.multiple_of(n * block + i * 16, 16), 16)
                one[spot] = first
                two[spot] = (value - first.astype(f32)).astype(bf16)
                return 0

            lax.fori_loop(0, block // 16, rows, 0, unroll=2)
            return 0

        lax.fori_loop(0, count, step, 0)

    shape = (1024, 2048)
    return call(
        body,
        [(shape, bf16)] * 2,
        (pltpu.with_memory_space_constraint(weights, pltpu.HBM),),
        scratch=[pltpu.VMEM((slots, block, 2048), f32), pltpu.SemaphoreType.DMA((slots,))],
        specs=[pl.BlockSpec(memory_space=pltpu.HBM)],
        limit=6 << 20,
        flops=1 << 24,
    )


def rows_to_lanes(total, rows):
    folded = total[:, :128] + total[:, 128:]
    lanes = []
    for start in range(0, rows, 128):
        block = folded[start : start + 128]
        if block.shape[0] < 128:
            block = jnp.concatenate([block, jnp.zeros((128 - block.shape[0], 128), f32)], axis=0)
        lanes.append(jnp.sum(block.T, axis=0, keepdims=True))
    lanes.append(jnp.zeros((8 - len(lanes), 128), f32))
    return jnp.concatenate(lanes, axis=0)


def lanes_to_rows(lanes, rows):
    blocks = []
    for i, start in enumerate(range(0, rows, 128)):
        count = min(128, rows - start)
        block = jnp.broadcast_to(lanes[i : i + 1], (128, 128)).T[:count]
        blocks.append(jnp.concatenate([block, block], axis=1))
    return blocks[0] if len(blocks) == 1 else jnp.concatenate(blocks, axis=0)


def product(orders, own, across, halves, rows, second_layer):
    extra = 8 if second_layer else 0

    def body(p, q, w1, w2, w3, w4, send, keep, lhs):
        core, col = lax.axis_index("row") % 2, lax.axis_index("col")

        def place(slot):
            mask = 0
            for i in range(3):
                dim = jnp.where(core == 0, orders[0][i], orders[1][i])
                mask = mask + ((slot >> (2 - i)) & 1) * dim
            y = col // 2
            y = jnp.where((mask & 1) == 1, y ^ 1, y)
            y = jnp.where((mask & 2) == 2, 3 - y, y)
            return y * 2 + ((col % 2) ^ (mask >> 2))

        total = None
        for m in range(8):
            ref = p.at[m] if m < 4 else q.at[m - 4]
            value = ref[:rows]
            if second_layer:
                total = value * value if total is None else total + value * value
                value = value * ref[rows : rows + 1]
            first = value.astype(bf16)
            lhs[:rows, m * F : (m + 1) * F] = first
            lhs[rows:, m * F : (m + 1) * F] = (value - first.astype(f32)).astype(bf16)

        def step(k, _):
            for target, slot in ((send, k + 4), (keep, k)):
                spot = pl.ds(pl.multiple_of(place(slot) * F, F), F)
                both = jnp.dot(lhs[:, :1024], w1[:, spot], preferred_element_type=f32)
                both = both + jnp.dot(lhs[:, 1024:], w3[:, spot], preferred_element_type=f32)
                other = jnp.dot(lhs[:rows, :1024], w2[:, spot], preferred_element_type=f32)
                other = other + jnp.dot(lhs[:rows, 1024:], w4[:, spot], preferred_element_type=f32)
                target[k, :rows] = both[:rows] + both[rows:] + other
            return 0

        lax.fori_loop(0, 4, step, 0, unroll=2)
        if second_layer:
            lanes = rows_to_lanes(total, rows)
            lanes = jnp.concatenate([lanes, jnp.zeros((8, 128), f32)], axis=1)
            for k in range(4):
                send[k, rows:] = lanes
                keep[k, rows:] = lanes

    return call(
        body,
        [((4, rows + extra, F), f32)] * 2,
        (own, across, *halves),
        scratch=[pltpu.VMEM((2 * rows, 2048), bf16)],
        limit=8 << 20,
        flops=6 * rows * 2048 * 2048,
    )


def add_halves(kept, arrived):
    half = kept.shape[0] // 2

    def body(keep, got, send, rest):
        send[...] = keep[half:] + got[half:]
        rest[...] = keep[:half] + got[:half]

    return call(body, [((half, *kept.shape[1:]), f32)] * 2, (kept, arrived), flops=1 << 20)


def summed(sent, kept, orders):
    for stage in range(3):
        if stage:
            sent, kept = add_halves(kept, arrived)
        arrived = swap_cols(sent, [order[stage] for order in orders])
    return kept, arrived


def gelu(z):
    return 0.5 * z * (1.0 + jnp.tanh(0.7978845608028654 * (z + 0.044715 * (z * z * z))))


def first_end(kept, arrived, gain, rows):
    def body(p, q, g, z, y):
        value = p[0] + q[0]
        z[...] = value
        y[:rows] = gelu(value)
        y[rows:] = jnp.broadcast_to(g[...], (8, F))

    return call(body, [((rows, F), f32), ((rows + 8, F), f32)], (kept, arrived, gain), flops=1 << 22)


def second_end(kept, arrived, before, gain, rows):
    def body(p, q, za, g, out, squares):
        section = lax.axis_index("section")
        lanes = (p[0, rows:] + q[0, rows:])[:, :128]
        scale = lax.rsqrt(lanes_to_rows(lanes, rows) / D + 1e-06)

        @pl.when(section == 0)
        def _():
            out[...] = gelu(za[...]) * scale * g[...]
            squares[...] = jnp.zeros((8, 128), f32)

        @pl.when(section != 0)
        def _():
            y = gelu(za[...] + scale * (p[0, :rows] + q[0, :rows]))
            squares[...] = rows_to_lanes(y * y, rows)
            out[...] = y * g[...]

    return call(
        body, [((rows, F), f32), ((8, 128), f32)], (kept, arrived, before, gain), flops=1 << 22
    )


def finish(values, lanes):
    count = len(values)
    sizes = [v.shape[0] for v in values]

    def body(*refs):
        section = lax.axis_index("section")
        lanes = refs[count]
        out = refs[count + 1]

        @pl.when(section == 0)
        def _():
            start = 0
            for ref, rows in zip(refs, sizes):
                out[start : start + rows] = ref[...]
                start += rows

        @pl.when(section != 0)
        def _():
            total = jnp.sum(lanes[...], axis=0, keepdims=True)
            start, place = 0, 0
            for ref, rows in zip(refs, sizes):
                width = -(-rows // 128)
                part = [total[:, (place + i) * 128 : (place + i + 1) * 128] for i in range(width)]
                scale = lax.rsqrt(lanes_to_rows(jnp.concatenate(part, axis=0), rows) / D + 1e-06)
                out[start : start + rows] = ref[...] * scale
                start += rows
                place += width

    return call(body, [((sum(sizes), F), f32)], (*values, lanes), flops=1 << 20)[0]


def joined(first, second):
    first = first.reshape(-1, *first.shape[-2:])
    second = second.reshape(-1, *second.shape[-2:])
    count = first.shape[0]

    def body(a, b, out):
        out[:count] = a[...]
        out[count:] = b[...]

    shape = (count + second.shape[0], *first.shape[1:])
    return call(body, [(shape, f32)], (first, second), flops=1 << 20)[0]


def gathered(value):
    first = swap_rows(value, [ring[0] for ring in RING])
    pair = joined(value, first)
    second = swap_rows(pair, [ring[1] for ring in RING])
    own = joined(pair, second)
    return own, swap_cores(own)


def chosen(own, moved):
    def body(a, b, out):
        out[...] = jnp.where(lax.axis_index("section") == 0, a[...], b[...])

    return call(body, [(own.shape, f32)], (own, moved))[0]


def pipeline(inputs, weights, norm_gain):
    flat = inputs.reshape(-1, F)
    gain = norm_gain
    halves = split_weights(weights.reshape(2048, 2048), 0)
    halves = halves + split_weights(weights.reshape(2048, 2048), 1)
    orders = [(CYCLE[i % 3], CYCLE[(i + 1) % 3]) for i in range(len(CHUNKS))]
    starts = [sum(CHUNKS[:i]) for i in range(len(CHUNKS))]

    before, branch = [], []
    for i, rows in enumerate(CHUNKS):
        own, across = gathered(flat[starts[i] : starts[i] + rows])
        sent, kept = product(orders[i], own, across, halves, rows, False)
        kept, arrived = summed(sent, kept, orders[i])
        z, y = first_end(kept, arrived, gain, rows)
        before.append(z)
        moved = lax.ppermute(y, "section", [(0, 1)])
        branch.append(chosen(y, moved))
    values, squares = [], []
    for i, rows in enumerate(CHUNKS):
        own, across = gathered(branch[i])
        sent, kept = product(orders[i], own, across, halves, rows, True)
        kept, arrived = summed(sent, kept, orders[i])
        value, square = second_end(kept, arrived, before[i], gain, rows)
        values.append(value)
        squares.append(square[: -(-rows // 128)].reshape(1, -1))
    lanes = jnp.concatenate(squares, axis=1)
    lanes = lax.all_to_all(jnp.broadcast_to(lanes[None], (64, *lanes.shape)), ("row", "col"), 0, 0, tiled=True)
    return finish(values, lanes.reshape(64, -1)).reshape(1, *inputs.shape)


def solution(mesh):
    placed = (
        P(None, None, ("row", "col")),
        P("section", None, "col", None, "row"),
        P("section", ("row", "col")),
    )
    return jax.shard_map(
        pipeline,
        mesh=mesh,
        in_specs=placed,
        out_specs=P("section", None, None, ("row", "col")),
        check_vma=False,
    )
```

```python
import jax
import jax.numpy as jnp
from jax import lax
from jax.experimental import pallas as pl
from jax.experimental.pallas import tpu as pltpu
from jax.sharding import PartitionSpec as P


CHUNKS = (144, 128, 112)
D = 16384
F = 256
f32 = jnp.float32
bf16 = jnp.bfloat16
CYCLE = ((4, 1, 2), (1, 2, 4), (2, 4, 1))
RING = ((1, 2), (2, 1))


def ring_partner(pos, mask):
    if mask & 1:
        pos = pos ^ 1
    if mask & 2:
        pos = 3 - pos
    return pos


def col_partner(col, mask):
    return ring_partner(col // 2, mask & 3) * 2 + ((col % 2) ^ (mask >> 2))


def swap_rows(value, masks):
    pairs = [(r, ring_partner(r // 2, masks[r % 2]) * 2 + r % 2) for r in range(8)]
    return lax.ppermute(value, "row", pairs)


def swap_cores(value):
    return lax.ppermute(value, "row", [(r, r ^ 1) for r in range(8)])


def swap_cols(value, masks):
    pairs = [(r * 8 + c, r * 8 + col_partner(c, masks[r % 2])) for r in range(8) for c in range(8)]
    return lax.ppermute(value, ("row", "col"), pairs)


def vmem():
    return pl.BlockSpec(memory_space=pltpu.VMEM)


def smem():
    return pl.BlockSpec(memory_space=pltpu.SMEM)


def call(body, outs, args, scratch=(), limit=4 << 20, scalars=0, flops=0, specs=None):
    return pl.pallas_call(
        body,
        out_shape=[jax.ShapeDtypeStruct(s, t) for s, t in outs],
        in_specs=specs or [smem()] * scalars + [vmem()] * (len(args) - scalars),
        out_specs=[vmem()] * len(outs),
        scratch_shapes=list(scratch),
        compiler_params=pltpu.CompilerParams(vmem_limit_bytes=limit),
        cost_estimate=pl.CostEstimate(flops=flops, transcendentals=0, bytes_accessed=0),
    )(*args)


def split_weights(weights, half):
    block, slots = 64, 8
    count = 1024 // block
    per = F // block

    def body(w, one, two, buf, sems):
        row = lax.axis_index("row")
        x, core = row // 2, row % 2

        def piece(m):
            whose = jnp.where(m < 4, core, 1 - core)
            low, high = m % 2, (m // 2) % 2
            one_flip = jnp.where(whose == 0, low, high)
            two_flip = jnp.where(whose == 0, high, low)
            chip = jnp.where(one_flip == 1, x ^ 1, x)
            chip = jnp.where(two_flip == 1, 3 - chip, chip)
            return chip * 2 + whose

        def fetch(n):
            m = n // per + 4 * half
            source = pl.multiple_of(piece(m) * F + (n % per) * block, block)
            return pltpu.make_async_copy(w.at[pl.ds(source, block)], buf.at[n % slots], sems.at[n % slots])

        for n in range(slots - 1):
            fetch(n).start()

        def step(n, _):
            @pl.when(n + slots - 1 < count)
            def _():
                fetch(n + slots - 1).start()

            fetch(n).wait()

            def rows(i, _):
                value = buf[n % slots, pl.ds(pl.multiple_of(i * 16, 16), 16)]
                first = value.astype(bf16)
                spot = pl.ds(pl.multiple_of(n * block + i * 16, 16), 16)
                one[spot] = first
                two[spot] = (value - first.astype(f32)).astype(bf16)
                return 0

            lax.fori_loop(0, block // 16, rows, 0, unroll=2)
            return 0

        lax.fori_loop(0, count, step, 0)

    shape = (1024, 2048)
    return call(
        body,
        [(shape, bf16)] * 2,
        (pltpu.with_memory_space_constraint(weights, pltpu.HBM),),
        scratch=[pltpu.VMEM((slots, block, 2048), f32), pltpu.SemaphoreType.DMA((slots,))],
        specs=[pl.BlockSpec(memory_space=pltpu.HBM)],
        limit=6 << 20,
        flops=1 << 24,
    )


def rows_to_lanes(total, rows):
    folded = total[:, :128] + total[:, 128:]
    lanes = []
    for start in range(0, rows, 128):
        block = folded[start : start + 128]
        if block.shape[0] < 128:
            block = jnp.concatenate([block, jnp.zeros((128 - block.shape[0], 128), f32)], axis=0)
        lanes.append(jnp.sum(block.T, axis=0, keepdims=True))
    lanes.append(jnp.zeros((8 - len(lanes), 128), f32))
    return jnp.concatenate(lanes, axis=0)


def lanes_to_rows(lanes, rows):
    blocks = []
    for i, start in enumerate(range(0, rows, 128)):
        count = min(128, rows - start)
        block = jnp.broadcast_to(lanes[i : i + 1], (128, 128)).T[:count]
        blocks.append(jnp.concatenate([block, block], axis=1))
    return blocks[0] if len(blocks) == 1 else jnp.concatenate(blocks, axis=0)


def product(orders, own, across, halves, rows, second_layer):
    extra = 8 if second_layer else 0

    def body(p, q, w1, w2, w3, w4, send, keep, lhs):
        core, col = lax.axis_index("row") % 2, lax.axis_index("col")

        def place(slot):
            mask = 0
            for i in range(3):
                dim = jnp.where(core == 0, orders[0][i], orders[1][i])
                mask = mask + ((slot >> (2 - i)) & 1) * dim
            y = col // 2
            y = jnp.where((mask & 1) == 1, y ^ 1, y)
            y = jnp.where((mask & 2) == 2, 3 - y, y)
            return y * 2 + ((col % 2) ^ (mask >> 2))

        total = None
        for m in range(8):
            ref = p.at[m] if m < 4 else q.at[m - 4]
            value = ref[:rows]
            if second_layer:
                total = value * value if total is None else total + value * value
                value = value * ref[rows : rows + 1]
            first = value.astype(bf16)
            lhs[:rows, m * F : (m + 1) * F] = first
            lhs[rows:, m * F : (m + 1) * F] = (value - first.astype(f32)).astype(bf16)

        def step(k):
            for target, slot in ((send, k + 4), (keep, k)):
                spot = pl.ds(pl.multiple_of(place(slot) * F, F), F)
                both = jnp.dot(lhs[:, :1024], w1[:, spot], preferred_element_type=f32)
                both = both + jnp.dot(lhs[:, 1024:], w3[:, spot], preferred_element_type=f32)
                other = jnp.dot(lhs[:rows, :1024], w2[:, spot], preferred_element_type=f32)
                other = other + jnp.dot(lhs[:rows, 1024:], w4[:, spot], preferred_element_type=f32)
                target[k, :rows] = both[:rows] + both[rows:] + other
            return 0

        for k in range(4):
            step(k)
        if second_layer:
            lanes = rows_to_lanes(total, rows)
            lanes = jnp.concatenate([lanes, jnp.zeros((8, 128), f32)], axis=1)
            for k in range(4):
                send[k, rows:] = lanes
                keep[k, rows:] = lanes

    return call(
        body,
        [((4, rows + extra, F), f32)] * 2,
        (own, across, *halves),
        scratch=[pltpu.VMEM((2 * rows, 2048), bf16)],
        limit=8 << 20,
        flops=6 * rows * 2048 * 2048,
    )


def add_halves(kept, arrived):
    half = kept.shape[0] // 2

    def body(keep, got, send, rest):
        send[...] = keep[half:] + got[half:]
        rest[...] = keep[:half] + got[:half]

    return call(body, [((half, *kept.shape[1:]), f32)] * 2, (kept, arrived), flops=1 << 20)


def summed(sent, kept, orders):
    for stage in range(3):
        if stage:
            sent, kept = add_halves(kept, arrived)
        arrived = swap_cols(sent, [order[stage] for order in orders])
    return kept, arrived


def gelu(z):
    return 0.5 * z * (1.0 + jnp.tanh(0.7978845608028654 * (z + 0.044715 * (z * z * z))))


def first_end(kept, arrived, gain, rows):
    def body(p, q, g, z, y):
        value = p[0] + q[0]
        z[...] = value
        y[:rows] = gelu(value)
        y[rows:] = jnp.broadcast_to(g[...], (8, F))

    return call(body, [((rows, F), f32), ((rows + 8, F), f32)], (kept, arrived, gain), flops=1 << 22)


def second_end(kept, arrived, before, gain, rows):
    def body(p, q, za, g, out, squares):
        section = lax.axis_index("section")
        lanes = (p[0, rows:] + q[0, rows:])[:, :128]
        scale = lax.rsqrt(lanes_to_rows(lanes, rows) / D + 1e-06)

        @pl.when(section == 0)
        def _():
            out[...] = gelu(za[...]) * scale * g[...]
            squares[...] = jnp.zeros((8, 128), f32)

        @pl.when(section != 0)
        def _():
            y = gelu(za[...] + scale * (p[0, :rows] + q[0, :rows]))
            squares[...] = rows_to_lanes(y * y, rows)
            out[...] = y * g[...]

    return call(
        body, [((rows, F), f32), ((8, 128), f32)], (kept, arrived, before, gain), flops=1 << 22
    )


def finish(values, lanes):
    count = len(values)
    sizes = [v.shape[0] for v in values]

    def body(*refs):
        section = lax.axis_index("section")
        lanes = refs[count]
        out = refs[count + 1]

        @pl.when(section == 0)
        def _():
            start = 0
            for ref, rows in zip(refs, sizes):
                out[start : start + rows] = ref[...]
                start += rows

        @pl.when(section != 0)
        def _():
            total = jnp.sum(lanes[...], axis=0, keepdims=True)
            start, place = 0, 0
            for ref, rows in zip(refs, sizes):
                width = -(-rows // 128)
                part = [total[:, (place + i) * 128 : (place + i + 1) * 128] for i in range(width)]
                scale = lax.rsqrt(lanes_to_rows(jnp.concatenate(part, axis=0), rows) / D + 1e-06)
                out[start : start + rows] = ref[...] * scale
                start += rows
                place += width

    return call(body, [((sum(sizes), F), f32)], (*values, lanes), flops=1 << 20)[0]


def joined(first, second):
    first = first.reshape(-1, *first.shape[-2:])
    second = second.reshape(-1, *second.shape[-2:])
    count = first.shape[0]

    def body(a, b, out):
        out[:count] = a[...]
        out[count:] = b[...]

    shape = (count + second.shape[0], *first.shape[1:])
    return call(body, [(shape, f32)], (first, second), flops=1 << 20)[0]


def gathered(value):
    first = swap_rows(value, [ring[0] for ring in RING])
    pair = joined(value, first)
    second = swap_rows(pair, [ring[1] for ring in RING])
    own = joined(pair, second)
    return own, swap_cores(own)


def chosen(own, moved):
    def body(a, b, out):
        out[...] = jnp.where(lax.axis_index("section") == 0, a[...], b[...])

    return call(body, [(own.shape, f32)], (own, moved))[0]


def pipeline(inputs, weights, norm_gain):
    flat = inputs.reshape(-1, F)
    gain = norm_gain
    halves = split_weights(weights.reshape(2048, 2048), 0)
    halves = halves + split_weights(weights.reshape(2048, 2048), 1)
    orders = [(CYCLE[i % 3], CYCLE[(i + 1) % 3]) for i in range(len(CHUNKS))]
    starts = [sum(CHUNKS[:i]) for i in range(len(CHUNKS))]

    before, branch = [], []
    for i, rows in enumerate(CHUNKS):
        own, across = gathered(flat[starts[i] : starts[i] + rows])
        sent, kept = product(orders[i], own, across, halves, rows, False)
        kept, arrived = summed(sent, kept, orders[i])
        z, y = first_end(kept, arrived, gain, rows)
        before.append(z)
        moved = lax.ppermute(y, "section", [(0, 1)])
        branch.append(chosen(y, moved))
    values, squares = [], []
    for i, rows in enumerate(CHUNKS):
        own, across = gathered(branch[i])
        sent, kept = product(orders[i], own, across, halves, rows, True)
        kept, arrived = summed(sent, kept, orders[i])
        value, square = second_end(kept, arrived, before[i], gain, rows)
        values.append(value)
        squares.append(square[: -(-rows // 128)].reshape(1, -1))
    lanes = jnp.concatenate(squares, axis=1)
    lanes = lax.all_to_all(jnp.broadcast_to(lanes[None], (64, *lanes.shape)), ("row", "col"), 0, 0, tiled=True)
    return finish(values, lanes.reshape(64, -1)).reshape(1, *inputs.shape)


def solution(mesh):
    placed = (
        P(None, None, ("row", "col")),
        P("section", None, "col", None, "row"),
        P("section", ("row", "col")),
    )
    return jax.shard_map(
        pipeline,
        mesh=mesh,
        in_specs=placed,
        out_specs=P("section", None, None, ("row", "col")),
        check_vma=False,
    )
```
